32 devices in a mesh: wave: 16 (over z, x, core), lev: 2 (over y).
Axes of the slice: x: 2, y: 2, z: 4, core: 2. Of those that a mesh axis runs over, the one named last changes fastest.
Arguments:
- spectral: float32 [136, 256, 2562], P('lev', 'wave'), may hold values from -6 to 6
- to_modes: float32 [136, 136], replicated, may hold values from -3 to 3
- from_modes: float32 [136, 136], replicated, may hold values from -3 to 3
- depth: float32 [136], replicated, may hold values from 0.02 to 50
- owner: int32 [128], replicated, may hold values from 0 to 15, as said below
Outputs:
- solved: float32 [136, 128, 2562], P('lev', 'wave')
The draws below stay inside these ranges and needn't reach their ends.
Inputs may be any that keep to these rules, and one draw needn't show every extreme that they name: `owner`: group q holds the pairs q * 1 to q * 1 + 1 - 1; a device stores its groups in increasing q from its first slot on, 1 slots each, and leaves its other slots unused. The 8 groups with the same q // 8 have 8 different owners. A device owns at most 16 groups, and some device exactly that many.
All inputs are finite; a program needn't handle non-finite values.
Results may differ from the reference program's by a relative error of at most 0.000075.
Values sent between devices are 32-bit elements; how exact they have to be, the bound alone decides.
No kernel may reach another device: no remote copies, remote signals or barrier semaphores. Data moves between devices by JAX's collectives and lax.ppermute only.
A program may use at most 128 MiB of HBM per device.

```python
import math
import jax
import jax.numpy as jnp
from jax import lax

NT = 1279
LEVELS = 136
KPAIR = 1
GROUPS = 8
PLEN = 1281
CAP = 16
PAIRS = 128
SLOTS = 256
NGROUPS = 128
N_WAVE = 16


def modes_matrix(key, salt):
    base = jax.random.fold_in(key, salt)
    first = jax.random.fold_in(base, 0)
    noise = jnp.clip(jax.random.normal(first, (LEVELS, LEVELS), jnp.float32), -4.0, 4.0)
    matrix = jnp.eye(LEVELS, dtype=jnp.float32) + 0.5 * noise / math.sqrt(LEVELS)
    return matrix


def draw_to_modes(key, part):
    return modes_matrix(key, 31)


def draw_from_modes(key, part):
    return modes_matrix(key, 47)


def draw_owner(key, part):
    first, second = jax.random.split(jax.random.fold_in(key, 11))
    half = N_WAVE // 2
    shifts = jax.random.randint(first, (half,), 0, GROUPS + 1).astype(jnp.int32)
    shifts = shifts.at[0].set(GROUPS)
    counts = jnp.concatenate([GROUPS + shifts, GROUPS - shifts])
    labels = jax.random.permutation(second, N_WAVE).astype(jnp.int32)
    bounds = jnp.cumsum(counts)
    positions = jnp.arange(NGROUPS, dtype=jnp.int32)
    runs = jnp.sum((positions[:, None] >= bounds[None, :]).astype(jnp.int32), axis=1)
    sequence = labels[runs]
    target = positions // GROUPS
    within = positions % GROUPS
    return sequence[within * N_WAVE + target].astype(jnp.int32)


def level_of(stream_key, dims, pieces, low, largest):
    factor_of, own = 1.0, jax.random.fold_in(stream_key, 6)
    for axis_at, parts in pieces:
        steps = jnp.exp(jax.random.uniform(jax.random.fold_in(own, axis_at), (parts,), jnp.float32, low / len(pieces), largest / len(pieces)))
        factor_of = factor_of * jnp.repeat(steps, dims[axis_at] // parts).reshape([-1 if axis == axis_at else 1 for axis in range(len(dims))])
    return factor_of


def scatter_about(own_key, shape, scale, bound, shards=(), kind=jnp.bfloat16):
    result = scale * jax.random.normal(own_key, shape, jnp.float32)
    if shards:
        result = result * level_of(own_key, shape, shards, -0.22, 0.18)
    return jnp.clip(result, -bound, bound).astype(kind)


def setup_inputs(seed: int = 0) -> dict:
    seeds = jax.random.split(jax.random.key(seed), 6)
    return {
        "spectral": scatter_about(seeds[0], (LEVELS, SLOTS, 2 * PLEN), 1.0, 6.0, ((0, 2), (1, 16)), jnp.float32),
        "to_modes": draw_to_modes(jax.random.fold_in(seeds[5], 71), 0),
        "from_modes": draw_from_modes(jax.random.fold_in(seeds[5], 71), 0),
        "depth": jnp.clip(jnp.exp(jax.random.uniform(seeds[3], (LEVELS,), jnp.float32, math.log(0.02), math.log(50.0))), 0.02, 50.0),
        "owner": draw_owner(jax.random.fold_in(seeds[5], 71), 0),
    }


def reference(spectral, to_modes, from_modes, depth, owner):
    numbers = jnp.arange(NGROUPS, dtype=jnp.int32)
    same = owner[:, None] == owner[None, :]
    rank = jnp.sum((same & (numbers[None, :] < numbers[:, None])).astype(jnp.int32), axis=1)
    first = owner * CAP + rank * KPAIR
    source = (first[:, None] + jnp.arange(KPAIR, dtype=jnp.int32)[None, :]).reshape(PAIRS).astype(jnp.int32)
    moved = jnp.take(spectral, source, axis=1)
    flat = moved.reshape(LEVELS, PAIRS * 2 * PLEN)
    pair = jnp.arange(PAIRS, dtype=jnp.int32)[:, None]
    column = jnp.arange(2 * PLEN, dtype=jnp.int32)[None, :]
    within = column % PLEN
    degree = jnp.where(within <= NT - pair, pair + within, within - 1)
    ratio = (degree * (degree + 1)).astype(jnp.float32) / float(NT * (NT + 1))
    ratio = ratio.reshape(PAIRS * 2 * PLEN)
    modes = jnp.dot(to_modes, flat, precision=lax.Precision.HIGHEST, preferred_element_type=jnp.float32)
    scaled = modes / (1.0 + depth[:, None] * ratio[None, :])
    solved = jnp.dot(from_modes, scaled, precision=lax.Precision.HIGHEST, preferred_element_type=jnp.float32)
    return solved.reshape(LEVELS, PAIRS, 2 * PLEN)
```

```python
import functools

import jax
import jax.numpy as jnp
from jax import lax
from jax.experimental import pallas as pl
from jax.experimental.pallas import tpu as pltpu
from jax.sharding import PartitionSpec as P

KPAIR = 1
LANES = 128
CHUNKS = (2, 3, 3, 2, 1)


def ranks_of(owner):
    numbers = jnp.arange(owner.shape[0], dtype=jnp.int32)
    same = owner[:, None] == owner[None, :]
    return jnp.sum((same & (numbers[None, :] < numbers[:, None])).astype(jnp.int32), axis=1)


def plain(spectral, to_modes, from_modes, depth, owner):
    waves = lax.axis_size("wave")
    groups = owner.shape[0] // waves
    own_index = lax.axis_index("wave")
    rank = ranks_of(owner)
    mine = owner == own_index
    pairs_target = own_index * groups * KPAIR + jnp.arange(groups * KPAIR, dtype=jnp.int32)
    offsets = jnp.arange(KPAIR, dtype=jnp.int32)
    first_slot = jnp.sum(jnp.where(mine, rank, 0).reshape(waves, groups), axis=1) * KPAIR
    picks = (first_slot[:, None] + offsets[None, :]).reshape(waves * KPAIR)
    outgoing = jnp.take(spectral, picks, axis=1)
    incoming = lax.all_to_all(outgoing, "wave", split_axis=1, concat_axis=1, tiled=True)
    senders = lax.dynamic_slice_in_dim(owner, own_index * groups, groups)
    places = (senders[:, None] * KPAIR + offsets[None, :]).reshape(groups * KPAIR)
    balanced = jnp.take(incoming, places, axis=1)
    level_rows, number, width = balanced.shape
    flat = balanced.reshape(level_rows, number * width)
    columns = lax.all_to_all(flat, "lev", split_axis=1, concat_axis=0, tiled=True)
    share = columns.shape[1]
    placed = lax.axis_index("lev") * share + jnp.arange(share, dtype=jnp.int32)
    top = width // 2 - 2
    within = placed % width % (top + 2)
    match = (placed // width)[None, :] == jnp.arange(number, dtype=jnp.int32)[:, None]
    pair = jnp.sum(jnp.where(match, pairs_target[:, None], 0), axis=0)
    degree = jnp.where(within <= top - pair, pair + within, within - 1)
    ratio = (degree * (degree + 1)).astype(jnp.float32) / float(top * (top + 1))
    modes = jnp.dot(to_modes, columns, precision=lax.Precision.HIGHEST, preferred_element_type=jnp.float32)
    scaled = modes / (1.0 + depth[:, None] * ratio[None, :])
    mixed = jnp.dot(from_modes, scaled, precision=lax.Precision.HIGHEST, preferred_element_type=jnp.float32)
    result = lax.all_to_all(mixed, "lev", split_axis=0, concat_axis=1, tiled=True)
    return result.reshape(level_rows, number, width)


def pack_kernel(levels, slots, width, first, picks_ref, even_ref, odd_ref, out_ref):
    start = (first + pl.program_id(0)) * 2 * LANES
    lane = lax.broadcasted_iota(jnp.int32, (levels, LANES), 1)
    for half, ref in enumerate((even_ref, odd_ref)):
        rows = ref.reshape(levels * slots, LANES)
        inside = lane + (start + half * LANES) < width
        for t in range(out_ref.shape[0]):
            part = rows[pl.ds(picks_ref[t], levels, slots), :]
            out_ref[t, pl.ds(half * levels, levels), :] = jnp.where(inside, part, 0.0)


def pack(spectral, picks, first, count):
    levels, slots, width = spectral.shape
    blocks = picks.shape[0]
    last = (width - 1) // LANES
    return pl.pallas_call(
        functools.partial(pack_kernel, levels, slots, width, first),
        grid_spec=pltpu.PrefetchScalarGridSpec(
            num_scalar_prefetch=1,
            grid=(count,),
            in_specs=[
                pl.BlockSpec((levels, slots, LANES), lambda i, s: (0, 0, 2 * (first + i))),
                pl.BlockSpec((levels, slots, LANES), lambda i, s: (0, 0, jnp.minimum(2 * (first + i) + 1, last))),
            ],
            out_specs=pl.BlockSpec((blocks, 2 * levels, LANES), lambda i, s: (0, i, 0)),
        ),
        out_shape=jax.ShapeDtypeStruct((blocks, count * 2 * levels, LANES), jnp.float32),
        cost_estimate=pl.CostEstimate(flops=0, bytes_accessed=count * blocks * levels * LANES * 16, transcendentals=0),
        name="pack",
    )(picks, spectral, spectral)


def choose_kernel(places_ref, in_ref, out_ref):
    out_ref[...] = in_ref[...]


def choose(received, places):
    _, rows, lanes = received.shape
    count = places.shape[0]
    return pl.pallas_call(
        choose_kernel,
        grid_spec=pltpu.PrefetchScalarGridSpec(
            num_scalar_prefetch=1,
            grid=(count,),
            in_specs=[pl.BlockSpec((1, rows, lanes), lambda i, s: (s[i], 0, 0))],
            out_specs=pl.BlockSpec((1, rows, lanes), lambda i, s: (i, 0, 0)),
        ),
        out_shape=jax.ShapeDtypeStruct((count, rows, lanes), jnp.float32),
        cost_estimate=pl.CostEstimate(flops=0, bytes_accessed=count * rows * lanes * 8, transcendentals=0),
        name="choose",
    )(places, received)


def split3(x, axis, order, reduce=False):
    short = lax.reduce_precision(x, 8, 7) if reduce else x.astype(jnp.bfloat16).astype(jnp.float32)
    high = short.astype(jnp.bfloat16)
    low = (x - short).astype(jnp.bfloat16)
    return jnp.concatenate([high if o else low for o in order], axis=axis)


def solve_kernel(levels, padded, width, first, lead_ref, to_ref, from_ref, depth_ref, own_ref, peer_ref, *refs):
    out_ref = refs[-1]
    number = own_ref.shape[0]
    half = pl.program_id(1)
    start = ((first + pl.program_id(0)) * 2 + half) * LANES
    top = width // 2 - 2

    @pl.when(start < width)
    def _():
        lane = lax.broadcasted_iota(jnp.int32, (1, LANES), 1)
        out_rows = out_ref.reshape(levels * number, LANES)
        base = pl.multiple_of(half * (2 * levels - padded), 8)
        own = jnp.concatenate([own_ref[p, pl.ds(base, padded), :] for p in range(number)], axis=1)
        peer = jnp.concatenate([peer_ref[p, pl.ds(base, padded), :] for p in range(number)], axis=1)
        both = jnp.concatenate([own, peer], axis=0)
        modes = jnp.dot(to_ref[half], split3(both, 0, (1, 0, 1)), preferred_element_type=jnp.float32)
        within = lax.rem(lane + start, top + 2)
        ratios = []
        for p in range(number):
            pair = lead_ref[0] + p
            degree = jnp.where(within <= top - pair, pair + within, within - 1)
            ratios.append((degree * (degree + 1)).astype(jnp.float32) / float(top * (top + 1)))
        ratio = jnp.concatenate(ratios, axis=1)
        scaled = modes / (1.0 + depth_ref[...] * ratio)
        mixed = jnp.dot(from_ref[...], split3(scaled, 0, (1, 0, 1)), preferred_element_type=jnp.float32)
        for p in range(number):
            out_rows[pl.ds(p, levels, number), :] = mixed[:levels, p * LANES : (p + 1) * LANES]


def solve(lead, to3, from3, depth2, own, peer, first, count, width, levels, total):
    number = own.shape[0]
    padded = (levels + 7) // 8 * 8
    last = (width - 1) // LANES
    ins = [lead, to3, from3, depth2, own, peer]
    block = pl.BlockSpec((number, 2 * levels, LANES), lambda i, j, s: (0, i, 0))
    specs = [
        pl.BlockSpec(to3.shape, lambda i, j, s: (0, 0, 0)),
        pl.BlockSpec(from3.shape, lambda i, j, s: (0, 0)),
        pl.BlockSpec(depth2.shape, lambda i, j, s: (0, 0)),
        block,
        block,
    ]
    alias = {}
    if total is not None:
        alias = {len(ins): 0}
        ins.append(total)
        specs.append(pl.BlockSpec(memory_space=pl.ANY))
    cells = count * number * 2 * LANES
    return pl.pallas_call(
        functools.partial(solve_kernel, levels, padded, width, first),
        grid_spec=pltpu.PrefetchScalarGridSpec(
            num_scalar_prefetch=1,
            grid=(count, 2),
            in_specs=specs,
            out_specs=pl.BlockSpec(
                (levels, number, LANES), lambda i, j, s: (0, 0, jnp.minimum(2 * (first + i) + j, last))
            ),
        ),
        out_shape=jax.ShapeDtypeStruct((levels, number, width), jnp.float32),
        input_output_aliases=alias,
        cost_estimate=pl.CostEstimate(flops=cells * levels * levels * 36, bytes_accessed=cells * levels * 12, transcendentals=0),
        name="solve",
    )(*ins)


def weights(to_modes, from_modes, depth, levels):
    modes = to_modes.shape[0]
    here = lax.axis_index("lev")
    padded = (levels + 7) // 8 * 8
    rows = (modes + 15) // 16 * 16
    own = lax.dynamic_slice_in_dim(to_modes, here * levels, levels, 1)
    peer = lax.dynamic_slice_in_dim(to_modes, (1 - here) * levels, levels, 1)
    extra = padded - levels
    tail = rows - modes
    first = jnp.concatenate([jnp.pad(own, ((0, tail), (0, extra))), jnp.pad(peer, ((0, tail), (0, extra)))], axis=1)
    second = jnp.concatenate([jnp.pad(own, ((0, tail), (extra, 0))), jnp.pad(peer, ((0, tail), (extra, 0)))], axis=1)
    to3 = split3(jnp.stack([first, second]), 2, (1, 1, 0), True)
    back = lax.dynamic_slice_in_dim(from_modes, here * levels, levels, 0)
    from3 = split3(jnp.pad(back, ((0, padded - levels), (0, tail))), 1, (1, 1, 0), True)
    return to3, from3, jnp.pad(depth, (0, tail), constant_values=1.0)[:, None]


def chunked(spectral, to_modes, from_modes, depth, owner):
    waves = lax.axis_size("wave")
    groups = owner.shape[0] // waves
    here = lax.axis_index("wave")
    levels, _, width = spectral.shape
    rank = ranks_of(owner)
    picks = jnp.sum(jnp.where(owner == here, rank, 0).reshape(waves, groups), axis=1)
    places = lax.dynamic_slice_in_dim(owner, here * groups, groups)
    lead = (here * groups).astype(jnp.int32).reshape(1)
    to3, from3, depth2 = weights(to_modes, from_modes, depth, levels)
    swap = [(0, 1), (1, 0)]
    total, first = None, 0
    for count in CHUNKS:
        outgoing = pack(spectral, picks, first, count)
        received = lax.all_to_all(outgoing, "wave", split_axis=0, concat_axis=0, tiled=True)
        own = choose(received, places)
        peer = lax.ppermute(own, "lev", swap)
        total = solve(lead, to3, from3, depth2, own, peer, first, count, width, levels, total)
        first += count
    return total


def per_device(spectral, to_modes, from_modes, depth, owner):
    fits = lax.axis_size("lev") == 2 and 2 * spectral.shape[0] % 8 == 0
    return (chunked if fits else plain)(spectral, to_modes, from_modes, depth, owner)


def solution(mesh):
    placed = (P("lev", "wave", None), P(), P(), P(), P())
    return jax.shard_map(
        per_device, mesh=mesh, in_specs=placed, out_specs=P("lev", "wave", None), check_vma=False
    )
```

```python
import functools

import jax
import jax.numpy as jnp
from jax import lax
from jax.experimental import pallas as pl
from jax.experimental.pallas import tpu as pltpu
from jax.sharding import PartitionSpec as P

KPAIR = 1
LANES = 128
CHUNKS = (1, 3, 2, 2, 1, 1)
VMEM = 16 * 2**20
LIMITS = (5, 6)
REST = 8
GROUPED = 2


def ranks_of(owner):
    numbers = jnp.arange(owner.shape[0], dtype=jnp.int32)
    same = owner[:, None] == owner[None, :]
    return jnp.sum((same & (numbers[None, :] < numbers[:, None])).astype(jnp.int32), axis=1)


def plain(spectral, to_modes, from_modes, depth, owner):
    waves = lax.axis_size("wave")
    groups = owner.shape[0] // waves
    own_index = lax.axis_index("wave")
    rank = ranks_of(owner)
    mine = owner == own_index
    pairs_target = own_index * groups * KPAIR + jnp.arange(groups * KPAIR, dtype=jnp.int32)
    offsets = jnp.arange(KPAIR, dtype=jnp.int32)
    first_slot = jnp.sum(jnp.where(mine, rank, 0).reshape(waves, groups), axis=1) * KPAIR
    picks = (first_slot[:, None] + offsets[None, :]).reshape(waves * KPAIR)
    outgoing = jnp.take(spectral, picks, axis=1)
    incoming = lax.all_to_all(outgoing, "wave", split_axis=1, concat_axis=1, tiled=True)
    senders = lax.dynamic_slice_in_dim(owner, own_index * groups, groups)
    places = (senders[:, None] * KPAIR + offsets[None, :]).reshape(groups * KPAIR)
    balanced = jnp.take(incoming, places, axis=1)
    level_rows, number, width = balanced.shape
    flat = balanced.reshape(level_rows, number * width)
    columns = lax.all_to_all(flat, "lev", split_axis=1, concat_axis=0, tiled=True)
    share = columns.shape[1]
    placed = lax.axis_index("lev") * share + jnp.arange(share, dtype=jnp.int32)
    top = width // 2 - 2
    within = placed % width % (top + 2)
    match = (placed // width)[None, :] == jnp.arange(number, dtype=jnp.int32)[:, None]
    pair = jnp.sum(jnp.where(match, pairs_target[:, None], 0), axis=0)
    degree = jnp.where(within <= top - pair, pair + within, within - 1)
    ratio = (degree * (degree + 1)).astype(jnp.float32) / float(top * (top + 1))
    modes = jnp.dot(to_modes, columns, precision=lax.Precision.HIGHEST, preferred_element_type=jnp.float32)
    scaled = modes / (1.0 + depth[:, None] * ratio[None, :])
    mixed = jnp.dot(from_modes, scaled, precision=lax.Precision.HIGHEST, preferred_element_type=jnp.float32)
    result = lax.all_to_all(mixed, "lev", split_axis=0, concat_axis=1, tiled=True)
    return result.reshape(level_rows, number, width)


def pack_kernel(levels, slots, rest, count, picks_ref, even_ref, odd_ref, out_ref):
    def row(ref, t):
        return ref.reshape(levels * slots, LANES)[pl.ds(picks_ref[t], levels, slots), :]

    @pl.when(pl.program_id(0) < count)
    def _():
        @pl.loop(0, out_ref.shape[0])
        def _(t):
            for half, ref in enumerate((even_ref, odd_ref)):
                out_ref[t, pl.ds(half * levels, levels), :] = row(ref, t)

    @pl.when(pl.program_id(0) == count)
    def _():
        kept = lax.broadcasted_iota(jnp.int32, (levels, LANES), 1) < rest

        @pl.loop(0, out_ref.shape[0])
        def _(t):
            tile = jnp.pad(jnp.where(kept, row(even_ref, t), 0.0), ((0, LANES - levels), (0, 0)))
            out_ref[t, pl.ds(0, REST), :] = tile.T[:REST]


def pack(spectral, picks, first, count, tail):
    levels, slots, width = spectral.shape
    blocks = picks.shape[0]
    last = (width - 1) // LANES
    rows = count * 2 * levels + tail * REST
    return pl.pallas_call(
        functools.partial(pack_kernel, levels, slots, width % (2 * LANES), count),
        grid_spec=pltpu.PrefetchScalarGridSpec(
            num_scalar_prefetch=1,
            grid=(count + tail,),
            in_specs=[
                pl.BlockSpec((levels, slots, LANES), lambda i, s: (0, 0, 2 * (first + i))),
                pl.BlockSpec((levels, slots, LANES), lambda i, s: (0, 0, jnp.minimum(2 * (first + i) + 1, last))),
            ],
            out_specs=pl.BlockSpec((blocks, 2 * levels, LANES), lambda i, s: (0, i, 0)),
        ),
        out_shape=pltpu.HBM((blocks, rows, LANES), jnp.float32),
        cost_estimate=pl.CostEstimate(flops=0, bytes_accessed=rows * blocks * LANES * 8, transcendentals=0),
        name="pack",
    )(picks, spectral, spectral)


def route_kernel(moves, inputs, table_ref, *refs):
    outs, sems = refs[inputs:-1], refs[-1]

    def copy(n):
        i, b, o = moves[n]
        slot = jnp.maximum(table_ref[n], 0)
        return pltpu.make_async_copy(refs[i].at[b], outs[o].at[slot], sems.at[n])

    for n in range(len(moves)):
        pl.when(table_ref[n] >= 0)(lambda n=n: copy(n).start())
    for n in range(len(moves)):
        pl.when(table_ref[n] >= 0)(lambda n=n: copy(n).wait())


def route(table, arrays, moves, sizes):
    _, rows, lanes = arrays[0].shape
    whole = pl.BlockSpec(memory_space=pltpu.VMEM)
    return pl.pallas_call(
        functools.partial(route_kernel, moves, len(arrays)),
        grid_spec=pltpu.PrefetchScalarGridSpec(
            num_scalar_prefetch=1,
            grid=(),
            in_specs=[pl.BlockSpec(memory_space=pltpu.HBM)] * len(arrays),
            out_specs=[whole] * len(sizes),
            scratch_shapes=[pltpu.SemaphoreType.DMA((len(moves),))],
        ),
        out_shape=[pltpu.HBM((n, rows, lanes), jnp.float32) for n in sizes],
        cost_estimate=pl.CostEstimate(flops=0, bytes_accessed=sum(sizes) * rows * lanes * 8, transcendentals=0),
        compiler_params=pltpu.CompilerParams(vmem_limit_bytes=VMEM),
    )(table, *arrays)


def split3(x, axis, order, reduce=False):
    short = lax.reduce_precision(x, 8, 7) if reduce else x.astype(jnp.bfloat16).astype(jnp.float32)
    high = short.astype(jnp.bfloat16)
    low = (x - short).astype(jnp.bfloat16)
    return jnp.concatenate([high if o else low for o in order], axis=axis)


def solve_kernel(levels, padded, width, first, count, lead_ref, to_ref, from_ref, depth_ref, own_ref, peer_ref, *refs):
    out_ref = refs[-1]
    number = own_ref.shape[0]
    step = pl.program_id(0)
    half = step % 2
    start = (first * 2 + step) * LANES
    top = width // 2 - 2
    lane = lax.broadcasted_iota(jnp.int32, (1, LANES), 1)
    out_rows = out_ref.reshape(levels * number, LANES)

    def ratio_of(pair, column):
        within = lax.rem(column, top + 2)
        degree = jnp.where(within <= top - pair, pair + within, within - 1)
        return (degree * (degree + 1)).astype(jnp.float32) / float(top * (top + 1))

    def apply(to, both, ratio):
        modes = jnp.dot(to, split3(both, 0, (1, 0, 1)), preferred_element_type=jnp.float32)
        scaled = modes / (1.0 + depth_ref[...] * ratio)
        return jnp.dot(from_ref[...], split3(scaled, 0, (1, 0, 1)), preferred_element_type=jnp.float32)

    @pl.when(step < 2 * count)
    def _():
        base = pl.multiple_of(half * (2 * levels - padded), 8)
        group = number // GROUPED

        @pl.loop(0, GROUPED)
        def _(g):
            pairs = [g * group + n for n in range(group)]
            own = jnp.concatenate([own_ref[p, pl.ds(base, padded), :] for p in pairs], axis=1)
            peer = jnp.concatenate([peer_ref[p, pl.ds(base, padded), :] for p in pairs], axis=1)
            ratio = jnp.concatenate([ratio_of(lead_ref[0] + p, lane + start) for p in pairs], axis=1)
            mixed = apply(to_ref[half], jnp.concatenate([own, peer], axis=0), ratio)
            for n, p in enumerate(pairs):
                out_rows[pl.ds(p, levels, number), :] = mixed[:levels, n * LANES : (n + 1) * LANES]

    @pl.when(step == 2 * count)
    def _():
        def levels_down(ref):
            tile = jnp.concatenate([ref[p, pl.ds(0, REST), :] for p in range(number)], axis=0)
            return jnp.pad(tile, ((0, LANES - number * REST), (0, 0))).T[:padded]

        ratio = ratio_of(lead_ref[0] + lane // REST, start + lane % REST)
        mixed = apply(to_ref[0], jnp.concatenate([levels_down(own_ref), levels_down(peer_ref)], axis=0), ratio)
        for p in range(number):
            shifted = mixed if p == 0 else pltpu.roll(mixed, LANES - p * REST, 1)
            out_rows[pl.ds(p, levels, number), :] = shifted[:levels]


def solve(lead, to3, from3, depth2, own, peer, first, count, tail, width, levels, total):
    number = own.shape[0]
    padded = (levels + 7) // 8 * 8
    ins = [lead, to3, from3, depth2, own, peer]
    block = pl.BlockSpec((number, 2 * levels, LANES), lambda i, s: (0, i // 2, 0))
    specs = [
        pl.BlockSpec(to3.shape, lambda i, s: (0, 0, 0)),
        pl.BlockSpec(from3.shape, lambda i, s: (0, 0)),
        pl.BlockSpec(depth2.shape, lambda i, s: (0, 0)),
        block,
        block,
    ]
    alias = {}
    if total is not None:
        alias = {len(ins): 0}
        ins.append(total)
        specs.append(pl.BlockSpec(memory_space=pl.ANY))
    cells = count * number * 2 * LANES
    return pl.pallas_call(
        functools.partial(solve_kernel, levels, padded, width, first, count),
        grid_spec=pltpu.PrefetchScalarGridSpec(
            num_scalar_prefetch=1,
            grid=(2 * count + tail,),
            in_specs=specs,
            out_specs=pl.BlockSpec((levels, number, LANES), lambda i, s: (0, 0, 2 * first + i)),
        ),
        out_shape=jax.ShapeDtypeStruct((levels, number, width), jnp.float32),
        input_output_aliases=alias,
        cost_estimate=pl.CostEstimate(flops=cells * levels * levels * 36, bytes_accessed=cells * levels * 12, transcendentals=0),
        compiler_params=pltpu.CompilerParams(vmem_limit_bytes=VMEM),
        name="solve",
    )(*ins)


def weights(to_modes, from_modes, depth, levels):
    modes = to_modes.shape[0]
    here = lax.axis_index("lev")
    padded = (levels + 7) // 8 * 8
    rows = (modes + 15) // 16 * 16
    own = lax.dynamic_slice_in_dim(to_modes, here * levels, levels, 1)
    peer = lax.dynamic_slice_in_dim(to_modes, (1 - here) * levels, levels, 1)
    extra = padded - levels
    tail = rows - modes
    first = jnp.concatenate([jnp.pad(own, ((0, tail), (0, extra))), jnp.pad(peer, ((0, tail), (0, extra)))], axis=1)
    second = jnp.concatenate([jnp.pad(own, ((0, tail), (extra, 0))), jnp.pad(peer, ((0, tail), (extra, 0)))], axis=1)
    to3 = split3(jnp.stack([first, second]), 2, (1, 1, 0), True)
    back = lax.dynamic_slice_in_dim(from_modes, here * levels, levels, 0)
    from3 = split3(jnp.pad(back, ((0, padded - levels), (0, tail))), 1, (1, 1, 0), True)
    return to3, from3, jnp.pad(depth, (0, tail), constant_values=1.0)[:, None]


PLANE = 4
PLANES = 4


def tables(owner, here):
    waves = lax.axis_size("wave")
    groups = owner.shape[0] // waves
    members = waves // 2
    half, mirror = here // members, here ^ (waves - PLANE)
    numbers = jnp.arange(owner.shape[0], dtype=jnp.int32)
    steps = jnp.arange(groups, dtype=jnp.int32)
    near = half * members + jnp.arange(members, dtype=jnp.int32)
    targets = jnp.stack([near, near ^ (waves - PLANE)], axis=1).reshape(waves)
    mine = (owner == here)[None, :]
    wanted = jnp.any(mine & (numbers // groups == targets[:, None]), axis=1)
    before = mine & (numbers[None, :] < (targets * groups)[:, None])
    picks = jnp.where(wanted, jnp.sum(before.astype(jnp.int32), axis=1), 0)
    earlier = steps[None, :] < steps[:, None]

    def place(target, same):
        owners = lax.dynamic_slice_in_dim(owner, target * groups, groups)
        kept = (owners // members == half) == same
        return owners, kept, jnp.sum((earlier & kept[None, :]).astype(jnp.int32), axis=1)

    def slots(owners, value):
        return jnp.sum(jnp.where(owners[None, :] == near[:, None], value[None, :] + 1, 0), axis=1) - 1

    owners, _, position = place(mirror, True)
    collect = slots(owners, position)
    owners, kept, position = place(here, False)
    hit = kept[None, :] & (position[None, :] == steps[:, None])
    gather = jnp.concatenate([slots(owners, steps), jnp.sum(jnp.where(hit, steps[None, :] + 1, 0), axis=1) - 1])
    crossing = owner // members != numbers // (groups * members)
    most = jnp.max(jnp.sum(crossing.astype(jnp.int32).reshape(waves, groups), axis=1))
    return picks, collect, gather, most


def chunked(spectral, to_modes, from_modes, depth, owner):
    waves = lax.axis_size("wave")
    groups = owner.shape[0] // waves
    members = waves // 2
    here = lax.axis_index("wave")
    levels, _, width = spectral.shape
    picks, collect, gather, most = tables(owner, here)
    lead = (here * groups).astype(jnp.int32).reshape(1)
    halves = [list(range(members)), list(range(members, waves))]
    mirrors = [(w, w ^ (waves - PLANE)) for w in range(waves)]

    rest = int(width % (2 * LANES) > 0)

    def relay(limit):
        to3, from3, depth2 = weights(to_modes, from_modes, depth, levels)
        total, first = None, 0
        for n, count in enumerate(CHUNKS):
            tail = rest if n == len(CHUNKS) - 1 else 0
            blocks = pack(spectral, picks, first, count, tail)
            shared = lax.all_to_all(blocks, "wave", 0, 0, axis_index_groups=halves, tiled=True)
            (chosen,) = route(collect, [shared], [(0, 2 * s + 1, 0) for s in range(members)], (limit,))
            crossed = lax.ppermute(chosen, "wave", mirrors)
            moves = [(0, 2 * s, 0) for s in range(members)] + [(1, i, 0) for i in range(limit)]
            (own,) = route(gather, [shared, crossed], moves, (groups,))
            peer = lax.ppermute(own, "lev", [(0, 1), (1, 0)])
            total = solve(lead, to3, from3, depth2, own, peer, first, count, tail, width, levels, total)
            first += count
        return total

    def branch(limit):
        def run():
            return relay(limit)

        return run

    limits = [k for k in LIMITS if k < groups] + [groups]
    level = sum((most > k).astype(jnp.int32) for k in limits[:-1])
    return lax.switch(level, [branch(k) for k in limits])


def per_device(spectral, to_modes, from_modes, depth, owner):
    planes = lax.axis_size("wave") // PLANE
    levels, _, width = spectral.shape
    fits = lax.axis_size("lev") == 2 and planes == PLANES and 2 * levels % 8 == 0 and levels <= LANES
    fits = fits and width // (2 * LANES) == sum(CHUNKS) and width % (2 * LANES) <= REST
    return (chunked if fits else plain)(spectral, to_modes, from_modes, depth, owner)


def solution(mesh):
    placed = (P("lev", "wave", None), P(), P(), P(), P())
    return jax.shard_map(
        per_device, mesh=mesh, in_specs=placed, out_specs=P("lev", "wave", None), check_vma=False
    )
```

```python
import functools

import jax
import jax.numpy as jnp
from jax import lax
from jax.experimental import pallas as pl
from jax.experimental.pallas import tpu as pltpu
from jax.sharding import PartitionSpec as P

KPAIR = 1
LANES = 128
CHUNKS = (1, 3, 2, 2, 1, 1)
BULK = (5, 5)
VMEM = 16 * 2**20
LIMITS = (5, 6)
REST = 8
GROUPED = 2


def ranks_of(owner):
    numbers = jnp.arange(owner.shape[0], dtype=jnp.int32)
    same = owner[:, None] == owner[None, :]
    return jnp.sum((same & (numbers[None, :] < numbers[:, None])).astype(jnp.int32), axis=1)


def plain(spectral, to_modes, from_modes, depth, owner):
    waves = lax.axis_size("wave")
    groups = owner.shape[0] // waves
    own_index = lax.axis_index("wave")
    rank = ranks_of(owner)
    mine = owner == own_index
    pairs_target = own_index * groups * KPAIR + jnp.arange(groups * KPAIR, dtype=jnp.int32)
    offsets = jnp.arange(KPAIR, dtype=jnp.int32)
    first_slot = jnp.sum(jnp.where(mine, rank, 0).reshape(waves, groups), axis=1) * KPAIR
    picks = (first_slot[:, None] + offsets[None, :]).reshape(waves * KPAIR)
    outgoing = jnp.take(spectral, picks, axis=1)
    incoming = lax.all_to_all(outgoing, "wave", split_axis=1, concat_axis=1, tiled=True)
    senders = lax.dynamic_slice_in_dim(owner, own_index * groups, groups)
    places = (senders[:, None] * KPAIR + offsets[None, :]).reshape(groups * KPAIR)
    balanced = jnp.take(incoming, places, axis=1)
    level_rows, number, width = balanced.shape
    flat = balanced.reshape(level_rows, number * width)
    columns = lax.all_to_all(flat, "lev", split_axis=1, concat_axis=0, tiled=True)
    share = columns.shape[1]
    placed = lax.axis_index("lev") * share + jnp.arange(share, dtype=jnp.int32)
    top = width // 2 - 2
    within = placed % width % (top + 2)
    match = (placed // width)[None, :] == jnp.arange(number, dtype=jnp.int32)[:, None]
    pair = jnp.sum(jnp.where(match, pairs_target[:, None], 0), axis=0)
    degree = jnp.where(within <= top - pair, pair + within, within - 1)
    ratio = (degree * (degree + 1)).astype(jnp.float32) / float(top * (top + 1))
    modes = jnp.dot(to_modes, columns, precision=lax.Precision.HIGHEST, preferred_element_type=jnp.float32)
    scaled = modes / (1.0 + depth[:, None] * ratio[None, :])
    mixed = jnp.dot(from_modes, scaled, precision=lax.Precision.HIGHEST, preferred_element_type=jnp.float32)
    result = lax.all_to_all(mixed, "lev", split_axis=0, concat_axis=1, tiled=True)
    return result.reshape(level_rows, number, width)


def pack_kernel(levels, slots, rest, count, picks_ref, even_ref, odd_ref, *out_refs):
    def row(ref, t):
        return ref.reshape(levels * slots, LANES)[pl.ds(picks_ref[t], levels, slots), :]

    each = out_refs[0].shape[0]

    @pl.when(pl.program_id(0) < count)
    def _():
        for n, out_ref in enumerate(out_refs):

            @pl.loop(0, each)
            def _(t):
                for half, ref in enumerate((even_ref, odd_ref)):
                    out_ref[t, pl.ds(half * levels, levels), :] = row(ref, n * each + t)

    @pl.when(pl.program_id(0) == count)
    def _():
        kept = lax.broadcasted_iota(jnp.int32, (levels, LANES), 1) < rest
        for n, out_ref in enumerate(out_refs):

            @pl.loop(0, each)
            def _(t):
                tile = jnp.pad(jnp.where(kept, row(even_ref, n * each + t), 0.0), ((0, LANES - levels), (0, 0)))
                out_ref[t, pl.ds(0, REST), :] = tile.T[:REST]


def pack(spectral, picks, first, count, tail, parts):
    levels, slots, width = spectral.shape
    blocks = picks.shape[0] // parts
    last = (width - 1) // LANES
    rows = count * 2 * levels + tail * REST
    return pl.pallas_call(
        functools.partial(pack_kernel, levels, slots, width % (2 * LANES), count),
        grid_spec=pltpu.PrefetchScalarGridSpec(
            num_scalar_prefetch=1,
            grid=(count + tail,),
            in_specs=[
                pl.BlockSpec((levels, slots, LANES), lambda i, s: (0, 0, 2 * (first + i))),
                pl.BlockSpec((levels, slots, LANES), lambda i, s: (0, 0, jnp.minimum(2 * (first + i) + 1, last))),
            ],
            out_specs=[pl.BlockSpec((blocks, 2 * levels, LANES), lambda i, s: (0, i, 0))] * parts,
        ),
        out_shape=[pltpu.HBM((blocks, rows, LANES), jnp.float32)] * parts,
        cost_estimate=pl.CostEstimate(flops=0, bytes_accessed=rows * blocks * parts * LANES * 8, transcendentals=0),
        name="pack",
    )(picks, spectral, spectral)


def route_kernel(moves, inputs, table_ref, *refs):
    outs, sems = refs[inputs:-1], refs[-1]

    def copy(n):
        i, b, o = moves[n]
        slot = jnp.maximum(table_ref[n], 0)
        return pltpu.make_async_copy(refs[i].at[b], outs[o].at[slot], sems.at[n])

    for n in range(len(moves)):
        pl.when(table_ref[n] >= 0)(lambda n=n: copy(n).start())
    for n in range(len(moves)):
        pl.when(table_ref[n] >= 0)(lambda n=n: copy(n).wait())


def route(table, arrays, moves, sizes):
    _, rows, lanes = arrays[0].shape
    whole = pl.BlockSpec(memory_space=pltpu.VMEM)
    return pl.pallas_call(
        functools.partial(route_kernel, moves, len(arrays)),
        grid_spec=pltpu.PrefetchScalarGridSpec(
            num_scalar_prefetch=1,
            grid=(),
            in_specs=[pl.BlockSpec(memory_space=pltpu.HBM)] * len(arrays),
            out_specs=[whole] * len(sizes),
            scratch_shapes=[pltpu.SemaphoreType.DMA((len(moves),))],
        ),
        out_shape=[pltpu.HBM((n, rows, lanes), jnp.float32) for n in sizes],
        cost_estimate=pl.CostEstimate(flops=0, bytes_accessed=sum(sizes) * rows * lanes * 8, transcendentals=0),
        compiler_params=pltpu.CompilerParams(vmem_limit_bytes=VMEM),
    )(table, *arrays)


def split3(x, axis, order, reduce=False):
    short = lax.reduce_precision(x, 8, 7) if reduce else x.astype(jnp.bfloat16).astype(jnp.float32)
    high = short.astype(jnp.bfloat16)
    low = (x - short).astype(jnp.bfloat16)
    return jnp.concatenate([high if o else low for o in order], axis=axis)


def solve_kernel(levels, padded, width, first, count, lead_ref, to_ref, from_ref, depth_ref, own_ref, peer_ref, *refs):
    out_ref = refs[-1]
    number = own_ref.shape[0]
    step = pl.program_id(0)
    half = step % 2
    start = (first * 2 + step) * LANES
    top = width // 2 - 2
    lane = lax.broadcasted_iota(jnp.int32, (1, LANES), 1)
    out_rows = out_ref.reshape(levels * number, LANES)

    def ratio_of(pair, column):
        within = lax.rem(column, top + 2)
        degree = jnp.where(within <= top - pair, pair + within, within - 1)
        return (degree * (degree + 1)).astype(jnp.float32) / float(top * (top + 1))

    def apply(to, both, ratio):
        modes = jnp.dot(to, split3(both, 0, (1, 0, 1)), preferred_element_type=jnp.float32)
        scaled = modes / (1.0 + depth_ref[...] * ratio)
        return jnp.dot(from_ref[...], split3(scaled, 0, (1, 0, 1)), preferred_element_type=jnp.float32)

    @pl.when(step < 2 * count)
    def _():
        base = pl.multiple_of(half * (2 * levels - padded), 8)
        group = number // GROUPED

        @pl.loop(0, GROUPED)
        def _(g):
            pairs = [g * group + n for n in range(group)]
            own = jnp.concatenate([own_ref[p, pl.ds(base, padded), :] for p in pairs], axis=1)
            peer = jnp.concatenate([peer_ref[p, pl.ds(base, padded), :] for p in pairs], axis=1)
            ratio = jnp.concatenate([ratio_of(lead_ref[0] + p, lane + start) for p in pairs], axis=1)
            mixed = apply(to_ref[half], jnp.concatenate([own, peer], axis=0), ratio)
            for n, p in enumerate(pairs):
                out_rows[pl.ds(p, levels, number), :] = mixed[:levels, n * LANES : (n + 1) * LANES]

    @pl.when(step == 2 * count)
    def _():
        def levels_down(ref):
            tile = jnp.concatenate([ref[p, pl.ds(0, REST), :] for p in range(number)], axis=0)
            return jnp.pad(tile, ((0, LANES - number * REST), (0, 0))).T[:padded]

        ratio = ratio_of(lead_ref[0] + lane // REST, start + lane % REST)
        mixed = apply(to_ref[0], jnp.concatenate([levels_down(own_ref), levels_down(peer_ref)], axis=0), ratio)
        for p in range(number):
            shifted = mixed if p == 0 else pltpu.roll(mixed, LANES - p * REST, 1)
            out_rows[pl.ds(p, levels, number), :] = shifted[:levels]


def solve(lead, to3, from3, depth2, own, peer, first, count, tail, width, levels, total):
    number = own.shape[0]
    padded = (levels + 7) // 8 * 8
    ins = [lead, to3, from3, depth2, own, peer]
    block = pl.BlockSpec((number, 2 * levels, LANES), lambda i, s: (0, i // 2, 0))
    specs = [
        pl.BlockSpec(to3.shape, lambda i, s: (0, 0, 0)),
        pl.BlockSpec(from3.shape, lambda i, s: (0, 0)),
        pl.BlockSpec(depth2.shape, lambda i, s: (0, 0)),
        block,
        block,
    ]
    alias = {}
    if total is not None:
        alias = {len(ins): 0}
        ins.append(total)
        specs.append(pl.BlockSpec(memory_space=pl.ANY))
    cells = count * number * 2 * LANES
    return pl.pallas_call(
        functools.partial(solve_kernel, levels, padded, width, first, count),
        grid_spec=pltpu.PrefetchScalarGridSpec(
            num_scalar_prefetch=1,
            grid=(2 * count + tail,),
            in_specs=specs,
            out_specs=pl.BlockSpec((levels, number, LANES), lambda i, s: (0, 0, 2 * first + i)),
        ),
        out_shape=jax.ShapeDtypeStruct((levels, number, width), jnp.float32),
        input_output_aliases=alias,
        cost_estimate=pl.CostEstimate(flops=cells * levels * levels * 36, bytes_accessed=cells * levels * 12, transcendentals=0),
        compiler_params=pltpu.CompilerParams(vmem_limit_bytes=VMEM),
        name="solve",
    )(*ins)


def weights(to_modes, from_modes, depth, levels):
    modes = to_modes.shape[0]
    here = lax.axis_index("lev")
    padded = (levels + 7) // 8 * 8
    rows = (modes + 15) // 16 * 16
    own = lax.dynamic_slice_in_dim(to_modes, here * levels, levels, 1)
    peer = lax.dynamic_slice_in_dim(to_modes, (1 - here) * levels, levels, 1)
    extra = padded - levels
    tail = rows - modes
    first = jnp.concatenate([jnp.pad(own, ((0, tail), (0, extra))), jnp.pad(peer, ((0, tail), (0, extra)))], axis=1)
    second = jnp.concatenate([jnp.pad(own, ((0, tail), (extra, 0))), jnp.pad(peer, ((0, tail), (extra, 0)))], axis=1)
    to3 = split3(jnp.stack([first, second]), 2, (1, 1, 0), True)
    back = lax.dynamic_slice_in_dim(from_modes, here * levels, levels, 0)
    from3 = split3(jnp.pad(back, ((0, padded - levels), (0, tail))), 1, (1, 1, 0), True)
    return to3, from3, jnp.pad(depth, (0, tail), constant_values=1.0)[:, None]


PLANE = 4
PLANES = 4


def tables(owner, here):
    waves = lax.axis_size("wave")
    groups = owner.shape[0] // waves
    members = waves // 2
    half, mirror = here // members, here ^ (waves - PLANE)
    numbers = jnp.arange(owner.shape[0], dtype=jnp.int32)
    steps = jnp.arange(groups, dtype=jnp.int32)
    near = here ^ jnp.arange(members, dtype=jnp.int32)
    targets = jnp.stack([near, near ^ (waves - PLANE)], axis=1).reshape(waves)
    mine = (owner == here)[None, :]
    wanted = jnp.any(mine & (numbers // groups == targets[:, None]), axis=1)
    before = mine & (numbers[None, :] < (targets * groups)[:, None])
    picks = jnp.where(wanted, jnp.sum(before.astype(jnp.int32), axis=1), 0)
    earlier = steps[None, :] < steps[:, None]

    def place(target, same):
        owners = lax.dynamic_slice_in_dim(owner, target * groups, groups)
        kept = (owners // members == half) == same
        return owners, kept, jnp.sum((earlier & kept[None, :]).astype(jnp.int32), axis=1)

    def slots(owners, value):
        return jnp.sum(jnp.where(owners[None, :] == near[:, None], value[None, :] + 1, 0), axis=1) - 1

    owners, _, position = place(mirror, True)
    collect = slots(owners, position)
    owners, kept, position = place(here, False)
    hit = kept[None, :] & (position[None, :] == steps[:, None])
    gather = jnp.concatenate([slots(owners, steps), jnp.sum(jnp.where(hit, steps[None, :] + 1, 0), axis=1) - 1])
    crossing = owner // members != numbers // (groups * members)
    most = jnp.max(jnp.sum(crossing.astype(jnp.int32).reshape(waves, groups), axis=1))
    return picks, collect, gather, most


def chunked(spectral, to_modes, from_modes, depth, owner):
    waves = lax.axis_size("wave")
    groups = owner.shape[0] // waves
    members = waves // 2
    here = lax.axis_index("wave")
    levels, _, width = spectral.shape
    picks, collect, gather, most = tables(owner, here)
    lead = (here * groups).astype(jnp.int32).reshape(1)
    mirrors = [(w, w ^ (waves - PLANE)) for w in range(waves)]

    rest = int(width % (2 * LANES) > 0)

    def relay(limit, chunks):
        to3, from3, depth2 = weights(to_modes, from_modes, depth, levels)
        total, first = None, 0
        for n, count in enumerate(chunks):
            tail = rest if n == len(chunks) - 1 else 0
            blocks = pack(spectral, picks, first, count, tail, members)
            shared = [blocks[0]]
            for e in range(1, members):
                shared.append(lax.ppermute(blocks[e], "wave", [(w, w ^ e) for w in range(waves)]))
            (chosen,) = route(collect, shared, [(s, 1, 0) for s in range(members)], (limit,))
            crossed = lax.ppermute(chosen, "wave", mirrors)
            moves = [(s, 0, 0) for s in range(members)] + [(members, i, 0) for i in range(limit)]
            (own,) = route(gather, [*shared, crossed], moves, (groups,))
            peer = lax.ppermute(own, "lev", [(0, 1), (1, 0)])
            total = solve(lead, to3, from3, depth2, own, peer, first, count, tail, width, levels, total)
            first += count
        return total

    def branch(limit):
        def run():
            return relay(limit, CHUNKS if limit < groups else BULK)

        return run

    limits = [k for k in LIMITS if k < groups] + [groups]
    level = sum((most > k).astype(jnp.int32) for k in limits[:-1])
    return lax.switch(level, [branch(k) for k in limits])


def per_device(spectral, to_modes, from_modes, depth, owner):
    planes = lax.axis_size("wave") // PLANE
    levels, _, width = spectral.shape
    fits = lax.axis_size("lev") == 2 and planes == PLANES and 2 * levels % 8 == 0 and levels <= LANES
    fits = fits and width // (2 * LANES) == sum(CHUNKS) and width % (2 * LANES) <= REST
    return (chunked if fits else plain)(spectral, to_modes, from_modes, depth, owner)


def solution(mesh):
    placed = (P("lev", "wave", None), P(), P(), P(), P())
    return jax.shard_map(
        per_device, mesh=mesh, in_specs=placed, out_specs=P("lev", "wave", None), check_vma=False
    )
```
